32 devices in a mesh: groups: 2 (over x), seq: 16 (over z, y, core).
Axes of the slice: x: 2, y: 2, z: 4, core: 2. Of those that a mesh axis runs over, the one named last changes fastest.
Arguments:
- queries: bfloat16 [4, 128, 8192], P(None, ('groups', 'seq')), parts along dimension 1, may hold values from -16 to 16
- new_keys: bfloat16 [4, 128, 1024], P(None, ('groups', 'seq')), parts along dimension 1, may hold values from -6 to 6
- new_values: bfloat16 [4, 128, 1024], P(None, ('groups', 'seq')), parts along dimension 1, may hold values from -6 to 6
- pool_keys: bfloat16 [2048, 16, 1024], P(('groups', 'seq')), parts along dimension 0, may hold values from -6 to 6
- pool_values: bfloat16 [2048, 16, 1024], P(('groups', 'seq')), parts along dimension 0, may hold values from -6 to 6
- page_table: int32 [128, 16], P(('groups', 'seq')), parts along dimension 0, may hold values from 0 to 63, as said below
- cached_len: int32 [128], P(('groups', 'seq')), parts along dimension 0, may hold values from 1 to 256
- turn_keys: bfloat16 [4, 32, 16, 1024], P(None, ('groups', 'seq')), parts along dimension 1, may hold values from -6 to 6
- turn_values: bfloat16 [4, 32, 16, 1024], P(None, ('groups', 'seq')), parts along dimension 1, may hold values from -6 to 6
- turn_lengths: int32 [32], P('groups'), parts along dimension 0, may hold values from 1 to 80, 768 in all
- turn_slot: int32 [32], P('groups'), parts along dimension 0, may hold values from 0 to 63, as said below
Outputs:
- attended: bfloat16 [4, 128, 8192], P(None, ('groups', 'seq')), parts along dimension 1
- landed_keys: bfloat16 [32, 80, 1024], P(('groups', 'seq')), parts along dimension 0
- landed_values: bfloat16 [32, 80, 1024], P(('groups', 'seq')), parts along dimension 0
The draws below stay inside these ranges and needn't reach their ends.
There are 2 independent parts, one for each index of `groups`. The reference program is written for one: setup_inputs(seed, part) draws one part's arguments, and reference() takes and returns one part's arrays. A program takes and returns all parts, laid end to end along the dimension named above; each array names one. Nothing has to cross between parts.
Inputs may be any that keep to these rules, and one draw needn't show every extreme that they name: `page_table`: the 4 rows of each device's slots together hold every number of 0 to 63 exactly once. `turn_lengths`: they sum to 768; the largest is exactly 80. `turn_slot`: each block of 4 slots holds the slot of exactly one turn.
All inputs are finite; a program needn't handle non-finite values.
Results may differ from the reference program's by a relative error of at most 0.0049.
Values may be sent and summed in bfloat16 or wider, within the bound.
A program may use at most 128 MiB of HBM per device.

```python
import math
import jax
import jax.numpy as jnp
import numpy as np
from jax import lax

QH = 64
KVH = 8
HD = 128
KV = 1024
PAGE = 16
STEPS = 4
SLOT_DEV = 4
CPAGES = 16
PG_DEV = 4
CHAIN = 16
TURNS = 16
SLOTS = 64
POOL_DEV = 64
POOL = 1024
PPAGES = 64
MOSTT = 80
TTOK = 768


key_level = 5.25


second_level = 5.21875


def draw_page_table(key, part):
    device_keys = jax.random.split(jax.random.fold_in(key, 11), CHAIN)

    def one_device(device_key):
        return jax.random.permutation(device_key, POOL_DEV)
    tables = jax.vmap(one_device)(device_keys)
    return tables.reshape(SLOTS, CPAGES).astype(jnp.int32)


def draw_turn_slot(key, part):
    owner_key, offset_key = jax.random.split(jax.random.fold_in(key, 23))
    owner_ids = jax.random.permutation(owner_key, CHAIN)[:TURNS]
    offsets = jax.random.randint(offset_key, (TURNS,), 0, SLOT_DEV)
    return (owner_ids * SLOT_DEV + offsets).astype(jnp.int32)


def drawn_parts(key):
    group_key, sign_key, level_key = jax.random.split(jax.random.fold_in(key, 77), 3)
    chosen = jax.random.randint(group_key, (SLOTS,), 0, KVH)
    signs = (2 * jax.random.randint(sign_key, (KVH, HD), 0, 2) - 1).astype(jnp.float32)
    levels = jax.random.uniform(level_key, (STEPS, SLOTS, QH // KVH), jnp.float32, 180.0, 320.0)
    return (chosen, signs, levels)


def base_draw(key, shape):
    return jax.random.truncated_normal(key, -6.0, 6.0, shape, jnp.float32)


def draw_queries(key, part):
    chosen, signs, levels = drawn_parts(key)
    group_share = QH // KVH
    base = base_draw(jax.random.fold_in(key, 5), (STEPS, SLOTS, KVH, group_share, HD))
    strength = levels / (key_level * math.sqrt(HD))
    planted = strength[:, :, None, :, None] * signs[None, None, :, None, :]
    in_group = jnp.arange(KVH)[None, :] == chosen[:, None]
    later = jnp.arange(STEPS) >= 1
    using = later[:, None, None] & in_group[None, :, :]
    mixed = jnp.where(using[..., None, None], planted, base)
    return mixed.reshape(STEPS, SLOTS, QH * HD).astype(jnp.bfloat16)


def draw_new_keys(key, part):
    chosen, signs, levels = drawn_parts(key)
    base = base_draw(jax.random.fold_in(key, 6), (STEPS, SLOTS, KVH, HD))
    step_level = jnp.where(jnp.arange(STEPS) == 0, key_level, second_level).astype(jnp.float32)
    planted = step_level[:, None, None, None] * signs[None, None, :, :]
    in_group = jnp.arange(KVH)[None, :] == chosen[:, None]
    early = jnp.arange(STEPS) <= 1
    using = early[:, None, None] & in_group[None, :, :]
    mixed = jnp.where(using[..., None], planted, base)
    return mixed.reshape(STEPS, SLOTS, KV).astype(jnp.bfloat16)


def plant(entries, own_key, least, high):
    place = [jax.random.randint(jax.random.fold_in(own_key, axis), (), 0, length) for axis, length in enumerate(entries.shape)]
    main_axis = entries.shape.index(max(entries.shape))
    next_to = place[:main_axis] + [(place[main_axis] + 1) % entries.shape[main_axis]] + place[main_axis + 1:]
    return entries.at[tuple(place)].set(least).at[tuple(next_to)].set(high)


def block_scale(own_key, extent, cuts, low, top_value):
    factor_of = 1.0
    for dim, parts in cuts:
        heights = jax.random.uniform(jax.random.fold_in(jax.random.fold_in(own_key, 6), dim), (parts,), jnp.float32, low / len(cuts), top_value / len(cuts))
        factor_of = factor_of * jnp.repeat(jnp.exp(heights), extent[dim] // parts).reshape((-1,) + (1,) * (len(extent) - 1 - dim))
    return factor_of


def split_up(number_of, total, most, skew):
    portions = [(1 << 20) // math.isqrt(grade ** skew) + 1 for grade in range(2, number_of + 1)]
    spare, counts = total - most - (number_of - 1), [1] * (number_of - 1)
    while spare > 0:
        movable = [i for i in range(number_of - 1) if counts[i] < most]
        pool, left = sum([portions[i] for i in movable]), spare
        for i in movable:
            addition = min(most - counts[i], max(1, left * portions[i] // pool), spare)
            counts[i] = counts[i] + addition
            spare = spare - addition
    return np.array([most] + counts)


def uneven(rng, count, total, limit, lean):
    if count == 2:
        one = jax.random.randint(rng, (), max(1, total - limit), min(limit, total - 1) + 1)
        return jnp.stack([one, total - one])
    sizes = jnp.asarray(split_up(count, total, limit, lean), jnp.int32)
    twos = (count - 1) // 2
    donor, receiver = sizes[1:1 + 2 * twos:2], sizes[2:2 + 2 * twos:2]
    slack = jnp.minimum(donor - 1, limit - receiver)
    passed = jax.random.randint(jax.random.fold_in(rng, 1), (twos,), 0, 1 << 20) % (slack + 1)
    sizes = sizes.at[1:1 + 2 * twos:2].set(donor - passed).at[2:2 + 2 * twos:2].set(receiver + passed)
    return sizes[jax.random.permutation(jax.random.fold_in(rng, 2), count)]


def normal_values(stream_key, extent, width, reach, pieces=(), held_as=jnp.bfloat16):
    drawn = jax.random.normal(stream_key, extent, jnp.float32) * width
    if len(pieces) > 0:
        drawn = block_scale(stream_key, extent, pieces, -0.22, 0.18) * drawn
    return jnp.clip(drawn, min=-reach, max=reach).astype(held_as)


def setup_inputs(seed: int = 0, part: int = 0) -> dict:
    streams_of = jax.random.split(jax.random.key(seed), 12)
    part_keys = jax.random.split(jax.random.fold_in(streams_of[11], part), 12)
    queries = draw_queries(jax.random.fold_in(jax.random.fold_in(streams_of[11], part), 71), part)
    new_keys = draw_new_keys(jax.random.fold_in(jax.random.fold_in(streams_of[11], part), 71), part)
    new_values = normal_values(part_keys[2], (STEPS, SLOTS, KV), 1.0, 6.0, ((1, 16),))
    pool_keys = normal_values(part_keys[3], (POOL, PAGE, KV), 1.0, 6.0, ((0, 16),))
    pool_values = normal_values(part_keys[4], (POOL, PAGE, KV), 1.0, 6.0, ((0, 16),))
    page_table = draw_page_table(jax.random.fold_in(jax.random.fold_in(streams_of[11], part), 71), part)
    cached_len = plant(jax.random.randint(part_keys[6], (SLOTS,), 1, CPAGES * PAGE + 1), jax.random.fold_in(part_keys[6], 1), 1, CPAGES * PAGE).astype(jnp.int32)
    turn_keys = normal_values(part_keys[7], (PG_DEV, CHAIN, PAGE, KV), 1.0, 6.0, ((1, 16),))
    turn_values = normal_values(part_keys[8], (PG_DEV, CHAIN, PAGE, KV), 1.0, 6.0, ((1, 16),))
    turn_lengths = uneven(part_keys[9], TURNS, TTOK, MOSTT, 2).astype(jnp.int32)
    turn_slot = draw_turn_slot(jax.random.fold_in(jax.random.fold_in(streams_of[11], part), 71), part)
    return {"queries": queries, "new_keys": new_keys, "new_values": new_values, "pool_keys": pool_keys, "pool_values": pool_values, "page_table": page_table, "cached_len": cached_len, "turn_keys": turn_keys, "turn_values": turn_values, "turn_lengths": turn_lengths, "turn_slot": turn_slot}


def reference(queries, new_keys, new_values, pool_keys, pool_values, page_table, cached_len, turn_keys, turn_values, turn_lengths, turn_slot):
    page_counts = (turn_lengths + PAGE - 1) // PAGE
    page_starts = jnp.cumsum(page_counts) - page_counts
    owner_ids = turn_slot // SLOT_DEV
    padding = jnp.zeros((MOSTT, KV), jnp.bfloat16)
    packed_keys = jnp.concatenate([turn_keys.reshape(PPAGES * PAGE, KV), padding], axis=0)
    packed_values = jnp.concatenate([turn_values.reshape(PPAGES * PAGE, KV), padding], axis=0)
    landed_keys = jnp.zeros((CHAIN, MOSTT, KV), jnp.bfloat16)
    landed_values = jnp.zeros((CHAIN, MOSTT, KV), jnp.bfloat16)
    positions = jnp.arange(MOSTT, dtype=jnp.int32)
    for turn_index in range(TURNS):
        first_token = (page_starts[turn_index] * PAGE).astype(jnp.int32)
        keeping = (positions < turn_lengths[turn_index])[:, None]
        piece_keys = lax.dynamic_slice_in_dim(packed_keys, first_token, MOSTT, 0)
        piece_values = lax.dynamic_slice_in_dim(packed_values, first_token, MOSTT, 0)
        landed_keys = landed_keys.at[owner_ids[turn_index]].set(jnp.where(keeping, piece_keys, jnp.zeros_like(piece_keys)))
        landed_values = landed_values.at[owner_ids[turn_index]].set(jnp.where(keeping, piece_values, jnp.zeros_like(piece_values)))
    slot_ids = jnp.arange(SLOTS, dtype=jnp.int32)
    matches = turn_slot[None, :] == slot_ids[:, None]
    fresh_lengths = lax.optimization_barrier(jnp.sum(jnp.where(matches, turn_lengths[None, :], 0), axis=1)).astype(jnp.int32)
    score_scale = 1.0 / math.sqrt(HD)
    group_share = QH // KVH
    token_span = CPAGES * PAGE
    causal_mask = jnp.arange(STEPS)[None, :] <= jnp.arange(STEPS)[:, None]

    def attend_slot(inputs):
        query_rows, key_rows, value_rows, table_row, resident_len, fresh_len, slot_id = inputs
        owner_id = slot_id // SLOT_DEV
        pool_rows = owner_id * POOL_DEV + table_row
        resident_keys = pool_keys[pool_rows].reshape(token_span, KV)
        resident_values = pool_values[pool_rows].reshape(token_span, KV)
        fresh_keys = lax.dynamic_index_in_dim(landed_keys, owner_id, 0, keepdims=False)
        fresh_values = lax.dynamic_index_in_dim(landed_values, owner_id, 0, keepdims=False)
        all_keys = jnp.concatenate([resident_keys, fresh_keys, key_rows], axis=0).astype(jnp.float32).reshape(-1, KVH, HD)
        all_values = jnp.concatenate([resident_values, fresh_values, value_rows], axis=0).astype(jnp.float32).reshape(-1, KVH, HD)
        valid_resident = jnp.broadcast_to((jnp.arange(token_span) < resident_len)[None, :], (STEPS, token_span))
        valid_fresh = jnp.broadcast_to((jnp.arange(MOSTT) < fresh_len)[None, :], (STEPS, MOSTT))
        valid_all = jnp.concatenate([valid_resident, valid_fresh, causal_mask], axis=1)
        query_heads = query_rows.astype(jnp.float32).reshape(STEPS, KVH, group_share, HD)
        scores = jnp.einsum('sgeh,cgh->sgec', query_heads, all_keys) * score_scale
        scores = jnp.where(valid_all[:, None, None, :], scores, -jnp.inf)
        largest = lax.optimization_barrier(jnp.max(scores, axis=-1, keepdims=True))
        weights = jnp.exp(scores - largest)
        weights = weights / lax.optimization_barrier(jnp.sum(weights, axis=-1, keepdims=True))
        mixed = jnp.einsum('sgec,cgh->sgeh', weights, all_values)
        return mixed.reshape(STEPS, QH * HD).astype(jnp.bfloat16)
    per_slot = lax.map(attend_slot, (jnp.swapaxes(queries, 0, 1), jnp.swapaxes(new_keys, 0, 1), jnp.swapaxes(new_values, 0, 1), page_table, cached_len, fresh_lengths, slot_ids))
    attended = jnp.swapaxes(per_slot, 0, 1)
    return (attended, landed_keys, landed_values)
```

```python
import functools
import math

import jax
import jax.numpy as jnp
from jax import lax
from jax.experimental import pallas as pl
from jax.experimental.pallas import tpu as pltpu
from jax.sharding import PartitionSpec as P

QH = 64
KVH = 8
HD = 128
MOSTT = 80
NEG = -1e30
F32 = jnp.float32
BF16 = jnp.bfloat16

FACTOR = math.log2(math.e) / math.sqrt(HD)


def scores_of(qb, g, keys, biases):
    share = QH // KVH
    parts = [qb[:, pl.ds((g * share + e) * HD, HD)] for e in range(share)]
    rows = jnp.concatenate(parts, axis=0)
    raw = lax.dot_general(rows, keys, (((1,), (1,)), ((), ())), preferred_element_type=F32)
    shaped = raw.reshape(share, biases.shape[0], keys.shape[0]) * FACTOR + biases[None]
    return shaped.reshape(rows.shape[0], keys.shape[0])


def each(first, last):
    if last - first > 32:
        return pl.loop(first, last)

    def run(body):
        for k in range(first, last):
            body(k)

    return run


def kernel(
    n,
    table_hbm,
    cached_hbm,
    lengths_hbm,
    slots_hbm,
    q_hbm,
    nk_hbm,
    nv_hbm,
    pk_hbm,
    pv_hbm,
    tk_hbm,
    tv_hbm,
    out_ref,
    lk_ref,
    lv_ref,
    qb,
    acc,
    mx,
    sm,
    pf,
    bias2_ref,
    q_v,
    n_v,
    pk_v,
    pv_v,
    t_v,
    first_k,
    first_v,
    second,
    landing,
    qf,
    table_ref,
    cached_ref,
    lengths_ref,
    slots_ref,
    start_s,
    pick_s,
    load_sem,
    send1,
    recv1,
    send2,
    recv2,
):
    me = lax.axis_index("seq")
    steps, slots_here, _ = q_hbm.shape
    group_pages, page_rows, kv_width = tk_hbm.shape
    pages_here = pk_hbm.shape[0]
    turns = lengths_ref.shape[0]
    cache_pages = table_ref.shape[1]
    spread = kv_width // HD
    most_pages = -(-MOSTT // page_rows)
    fresh_span = most_pages * page_rows
    rows_sr = steps * slots_here
    share = QH // KVH
    mine = lax.rem(me, spread)
    base = me - mine
    first = (first_k, first_v)

    barrier = pltpu.get_barrier_semaphore()

    @each(1, n)
    def _(k):
        pl.semaphore_signal(barrier, inc=1, device_id={"seq": lax.rem(me + k, n)})

    def load(index, src, dst):
        return pltpu.make_async_copy(src, dst, load_sem.at[index])

    loads = [
        load(0, tk_hbm, t_v.at[0]),
        load(1, tv_hbm, t_v.at[1]),
        load(2, q_hbm, q_v),
        load(3, pk_hbm, pk_v),
        load(4, pv_hbm, pv_v),
        load(5, nk_hbm, n_v.at[0]),
        load(6, nv_hbm, n_v.at[1]),
        load(7, lengths_hbm, lengths_ref),
        load(8, slots_hbm, slots_ref),
        load(9, table_hbm, table_ref),
        load(10, cached_hbm, cached_ref),
    ]
    for copy in loads:
        copy.start()

    def hand1(a, k):
        d = lax.rem(me + k, n)
        left = pl.multiple_of(lax.rem(d, spread) * HD, HD)
        return pltpu.make_async_remote_copy(
            src_ref=t_v.at[a, :, :, pl.ds(left, HD)],
            dst_ref=first[a].at[pl.ds(me * group_pages, group_pages)],
            send_sem=send1.at[a, k],
            recv_sem=recv1.at[a, k],
            device_id={"seq": d},
        )

    def hand2(a, k):
        to = lax.rem(mine + k, spread)
        return pltpu.make_async_remote_copy(
            src_ref=second.at[a, to],
            dst_ref=landing.at[a, mine, pl.ds(0, most_pages)],
            send_sem=send2.at[a, k],
            recv_sem=recv2.at[a, k],
            device_id={"seq": base + to},
        )

    pl.semaphore_wait(barrier, n - 1)
    left_mine = pl.multiple_of(mine * HD, HD)
    for a in range(2):
        loads[a].wait()

        @each(1, n)
        def _(k, a=a):
            hand1(a, k).start()

    for a in range(2):
        for p in range(group_pages):
            first[a][me * group_pages + p] = t_v[a, p, :, pl.ds(left_mine, HD)]

    for copy in loads[7:]:
        copy.wait()
    running = jnp.int32(0)
    my_length = jnp.int32(0)
    my_slot = jnp.int32(0)
    for t in range(turns):
        start_s[t] = running
        length = lengths_ref[t]
        slot = slots_ref[t]
        own = lax.div(slot, slots_here) == me
        my_length = jnp.where(own, length, my_length)
        my_slot = jnp.where(own, lax.rem(slot, slots_here), my_slot)
        running = running + lax.div(length + (page_rows - 1), page_rows)

    for to in range(spread):
        begin = jnp.int32(0)
        for t in range(turns):
            begin = jnp.where(lax.div(slots_ref[t], slots_here) == base + to, start_s[t], begin)
        for j in range(most_pages):
            page = jnp.minimum(begin + j, group_pages * n - 1)
            pick_s[to * most_pages + j] = lax.rem(page, n) * group_pages + lax.div(page, n)

    loads[2].wait()
    for s in range(steps):
        qf[pl.ds(s * slots_here, slots_here), :] = q_v[s].astype(F32)
    qb[...] = qf[...].astype(BF16)

    tokens = pages_here * page_rows
    col = lax.broadcasted_iota(jnp.int32, (1, tokens), 1)
    col_page = col // page_rows
    col_row = col % page_rows
    lines = []
    for r in range(slots_here):
        room = jnp.zeros((1, tokens), jnp.int32)
        for c in range(cache_pages):
            left_over = cached_ref[r] - c * page_rows
            room = jnp.where(col_page == table_ref[r, c], left_over, room)
        lines.append(jnp.where(col_row < room, 0.0, NEG).astype(F32))
    bias = jnp.concatenate(lines * (rows_sr // slots_here), axis=0)

    def resident(g):
        keys = pk_v[:, :, pl.ds(g * HD, HD)].reshape(tokens, HD)
        values = pv_v[:, :, pl.ds(g * HD, HD)].reshape(tokens, HD)
        score = scores_of(qb, g, keys, bias)
        largest = jnp.max(score, axis=-1, keepdims=True)
        prob = jnp.exp2(score - largest)
        mx[:, g : g + 1] = largest
        sm[:, g : g + 1] = jnp.sum(prob, axis=-1, keepdims=True)
        acc[g] = jnp.dot(prob.astype(BF16), values, preferred_element_type=F32)

    loads[3].wait()
    loads[4].wait()
    for g in range(KVH):
        resident(g)

    loads[5].wait()
    loads[6].wait()
    for a in range(2):
        rows = jnp.concatenate([n_v[a, s].astype(F32) for s in range(steps)], axis=0).astype(BF16)
        for g in range(KVH):
            landing[a, g, most_pages] = rows[:, g * HD : (g + 1) * HD]
    extra = fresh_span + rows_sr
    line = lax.broadcasted_iota(jnp.int32, (rows_sr, extra), 0)
    col = lax.broadcasted_iota(jnp.int32, (rows_sr, extra), 1)
    line_slot, line_step = line % slots_here, line // slots_here
    new_at = jnp.maximum(col - fresh_span, 0)
    fine_fresh = (line_slot == my_slot) & (col < my_length)
    fine_new = (
        (col >= fresh_span)
        & (new_at % slots_here == line_slot)
        & (new_at // slots_here <= line_step)
    )
    bias2_ref[...] = jnp.where(fine_fresh | fine_new, 0.0, NEG).astype(F32)

    def pass_on(a):
        @each(1, n)
        def _(k):
            hand1(a, k).wait_recv()

        for k in range(1, spread):
            to = lax.rem(mine + k, spread)
            for j in range(most_pages):
                second[a, to, j] = first[a][pick_s[to * most_pages + j]]
            hand2(a, k).start()
        for j in range(most_pages):
            landing[a, mine, j] = first[a][pick_s[mine * most_pages + j]]

    place = lax.broadcasted_iota(jnp.int32, (page_rows, HD), 0)

    def land(a, ref, g):
        for j in range(most_pages):
            page = landing[a, g, j].astype(F32)
            kept = jnp.where(place + j * page_rows < my_length, page, 0.0)
            ref[j, :, pl.ds(g * HD, HD)] = kept.astype(BF16)

    pass_on(0)
    for k in range(1, spread):
        hand2(0, k).wait_recv()
    bias2 = bias2_ref[...]
    for g in range(KVH):
        score = scores_of(qb, g, landing[0, g].reshape(extra, HD), bias2)
        before = mx[:, g : g + 1]
        largest = jnp.maximum(before, jnp.max(score, axis=-1, keepdims=True))
        prob = jnp.exp2(score - largest)
        shrink = jnp.exp2(before - largest)
        total = sm[:, g : g + 1] * shrink + jnp.sum(prob, axis=-1, keepdims=True)
        inverse = 1.0 / total
        acc[g] = acc[g] * (shrink * inverse)
        pf[g] = (prob * inverse).astype(BF16)
        land(0, lk_ref, g)

    pass_on(1)
    for k in range(1, spread):
        hand2(1, k).wait_recv()
    for g in range(KVH):
        values = landing[1, g].reshape(extra, HD)
        result = acc[g] + jnp.dot(pf[g], values, preferred_element_type=F32)
        for e in range(share):
            qf[:, pl.ds((g * share + e) * HD, HD)] = result[e * rows_sr : (e + 1) * rows_sr]
        land(1, lv_ref, g)
    for s in range(steps):
        out_ref[s] = qf[pl.ds(s * slots_here, slots_here), :].astype(BF16)

    for a in range(2):

        @each(1, n)
        def _(k, a=a):
            hand1(a, k).wait_send()

        for k in range(1, spread):
            hand2(a, k).wait_send()


def store(a_ref, b_ref, c_ref, a_hbm, b_hbm, c_hbm, sem):
    copies = [
        pltpu.make_async_copy(src, dst, sem.at[i])
        for i, (src, dst) in enumerate(((a_ref, a_hbm), (b_ref, b_hbm), (c_ref, c_hbm)))
    ]
    for copy in copies:
        copy.start()
    for copy in copies:
        copy.wait()


def per_device(
    queries,
    new_keys,
    new_values,
    pool_keys,
    pool_values,
    page_table,
    cached_len,
    turn_keys,
    turn_values,
    turn_lengths,
    turn_slot,
):
    n = lax.axis_size("seq")
    steps, slots_here, query_width = queries.shape
    pages_here, page_rows, kv_width = pool_keys.shape
    group_pages = turn_keys.shape[0]
    most_pages = -(-MOSTT // page_rows)
    spread = kv_width // HD
    rows_sr = steps * slots_here
    rows = rows_sr * (QH // KVH)
    paged = (group_pages, page_rows, kv_width)
    hbm = pl.BlockSpec(memory_space=pltpu.HBM)
    vmem = pl.BlockSpec(memory_space=pltpu.VMEM)
    extra = most_pages * page_rows + rows_sr
    landed = jax.ShapeDtypeStruct((most_pages, page_rows, kv_width), BF16)
    outs = (jax.ShapeDtypeStruct(queries.shape, BF16), landed, landed)
    held = [
        pltpu.with_memory_space_constraint(x, pltpu.HBM)
        for x in (
            page_table,
            cached_len,
            turn_lengths,
            turn_slot,
            queries,
            new_keys,
            new_values,
            pool_keys,
            pool_values,
            turn_keys.reshape(paged),
            turn_values.reshape(paged),
        )
    ]
    parts = pl.pallas_call(
        functools.partial(kernel, n),
        out_shape=outs,
        in_specs=[hbm] * 11,
        out_specs=(vmem,) * 3,
        scratch_shapes=[
            pltpu.VMEM((rows_sr, query_width), BF16),
            pltpu.VMEM((KVH, rows, HD), F32),
            pltpu.VMEM((rows, KVH), F32),
            pltpu.VMEM((rows, KVH), F32),
            pltpu.VMEM((KVH, rows, extra), BF16),
            pltpu.VMEM((rows_sr, extra), F32),
            pltpu.VMEM(queries.shape, BF16),
            pltpu.VMEM((2,) + new_keys.shape, BF16),
            pltpu.VMEM(pool_keys.shape, BF16),
            pltpu.VMEM(pool_values.shape, BF16),
            pltpu.VMEM((2,) + paged, BF16),
            pltpu.VMEM((n * group_pages, page_rows, HD), BF16),
            pltpu.VMEM((n * group_pages, page_rows, HD), BF16),
            pltpu.VMEM((2, spread, most_pages, page_rows, HD), BF16),
            pltpu.VMEM((2, spread, most_pages + 1, page_rows, HD), BF16),
            pltpu.VMEM((rows_sr, query_width), F32),
            pltpu.SMEM(page_table.shape, jnp.int32),
            pltpu.SMEM(cached_len.shape, jnp.int32),
            pltpu.SMEM(turn_lengths.shape, jnp.int32),
            pltpu.SMEM(turn_slot.shape, jnp.int32),
            pltpu.SMEM(turn_lengths.shape, jnp.int32),
            pltpu.SMEM((spread * most_pages,), jnp.int32),
            pltpu.SemaphoreType.DMA((11,)),
            pltpu.SemaphoreType.DMA((2, n)),
            pltpu.SemaphoreType.DMA((2, n)),
            pltpu.SemaphoreType.DMA((2, spread)),
            pltpu.SemaphoreType.DMA((2, spread)),
        ],
        compiler_params=pltpu.CompilerParams(
            collective_id=0, has_side_effects=True, vmem_limit_bytes=24 * 1024 * 1024
        ),
    )(*held)
    attended, landed_keys, landed_values = pl.pallas_call(
        store,
        out_shape=outs,
        in_specs=[vmem] * 3,
        out_specs=(hbm,) * 3,
        scratch_shapes=[pltpu.SemaphoreType.DMA((3,))],
        compiler_params=pltpu.CompilerParams(vmem_limit_bytes=8 * 1024 * 1024),
    )(*parts)
    span = most_pages * page_rows
    return (
        attended,
        landed_keys.reshape(1, span, kv_width),
        landed_values.reshape(1, span, kv_width),
    )


def solution(mesh):
    in_specs = (
        P(None, ("groups", "seq"), None),
        P(None, ("groups", "seq"), None),
        P(None, ("groups", "seq"), None),
        P(("groups", "seq"), None, None),
        P(("groups", "seq"), None, None),
        P(("groups", "seq"), None),
        P(("groups", "seq")),
        P(None, ("groups", "seq"), None, None),
        P(None, ("groups", "seq"), None, None),
        P("groups"),
        P("groups"),
    )
    out_specs = (
        P(None, ("groups", "seq"), None),
        P(("groups", "seq"), None, None),
        P(("groups", "seq"), None, None),
    )
    return jax.shard_map(
        per_device, mesh=mesh, in_specs=in_specs, out_specs=out_specs, check_vma=False
    )
```

```python
import functools
import math

import jax
import jax.numpy as jnp
from jax import lax
from jax.experimental import pallas as pl
from jax.experimental.pallas import tpu as pltpu
from jax.sharding import PartitionSpec as P

QH = 64
KVH = 8
HD = 128
MOSTT = 80
SUB = 8
NEG = -1e30
F32 = jnp.float32
BF16 = jnp.bfloat16

FACTOR = math.log2(math.e) / math.sqrt(HD)


def scores_of(qb, g, keys, biases):
    share = QH // KVH
    parts = [qb[:, pl.ds((g * share + e) * HD, HD)] for e in range(share)]
    rows = jnp.concatenate(parts, axis=0)
    raw = lax.dot_general(rows, keys, (((1,), (1,)), ((), ())), preferred_element_type=F32)
    shaped = raw.reshape(share, biases.shape[0], keys.shape[0]) * FACTOR + biases[None]
    return shaped.reshape(rows.shape[0], keys.shape[0])


def each(first, last):
    if last - first > 32:
        return pl.loop(first, last)

    def run(body):
        for k in range(first, last):
            body(k)

    return run


def kernel(
    n,
    table_hbm,
    cached_hbm,
    lengths_hbm,
    slots_hbm,
    q_hbm,
    nk_hbm,
    nv_hbm,
    pk_hbm,
    pv_hbm,
    tk_hbm,
    tv_hbm,
    out_ref,
    lk_ref,
    lv_ref,
    qb,
    acc,
    mx,
    sm,
    pf,
    bias2_ref,
    q_v,
    n_v,
    pk_v,
    pv_v,
    t_v,
    first_k,
    first_v,
    second,
    landing,
    fresh,
    qf,
    table_ref,
    cached_ref,
    lengths_ref,
    slots_ref,
    start_s,
    pick_s,
    load_sem,
    own_sem,
    send1,
    recv1,
    send2,
    recv2,
):
    me = lax.axis_index("seq")
    steps, slots_here, _ = q_hbm.shape
    group_pages, page_rows, kv_width = tk_hbm.shape
    pages_here = pk_hbm.shape[0]
    turns = lengths_ref.shape[0]
    cache_pages = table_ref.shape[1]
    lane_tiles = kv_width // HD
    spread = (page_rows // SUB) * lane_tiles
    most_pages = -(-MOSTT // page_rows)
    fresh_span = most_pages * page_rows
    blocks = n // spread
    rows_sr = steps * slots_here
    share = QH // KVH
    my_block = me // spread
    first = (first_k, first_v)
    if blocks == 1:
        fresh = landing.at[:, 0]

    barrier = pltpu.get_barrier_semaphore()

    @each(1, n)
    def _(k):
        pl.semaphore_signal(barrier, inc=1, device_id={"seq": lax.rem(me + k, n)})

    def load(index, src, dst):
        return pltpu.make_async_copy(src, dst, load_sem.at[index])

    loads = [
        load(0, tk_hbm, t_v.at[0]),
        load(1, tv_hbm, t_v.at[1]),
        load(2, q_hbm, q_v),
        load(3, pk_hbm, pk_v),
        load(4, pv_hbm, pv_v),
        load(5, nk_hbm, n_v.at[0]),
        load(6, nv_hbm, n_v.at[1]),
        load(7, lengths_hbm, lengths_ref),
        load(8, slots_hbm, slots_ref),
        load(9, table_hbm, table_ref),
        load(10, cached_hbm, cached_ref),
    ]
    for copy in loads:
        copy.start()

    def tile(h):
        t = lax.rem(h, spread)
        top = pl.multiple_of(lax.div(t, lane_tiles) * SUB, SUB)
        return pl.ds(top, SUB), lax.rem(t, lane_tiles)

    def tile_of(a, h):
        top, head = tile(h)
        return t_v.at[a, :, top, pl.ds(pl.multiple_of(head * HD, HD), HD)]

    def slot_of(src):
        return pl.ds(lax.rem(src, spread) * group_pages, group_pages)

    def hand1(a, k):
        h = my_block * spread + lax.rem(lax.rem(me, spread) + k, spread)
        return pltpu.make_async_remote_copy(
            src_ref=tile_of(a, h),
            dst_ref=first[a].at[slot_of(me)],
            send_sem=send1.at[a, k],
            recv_sem=recv1.at[a, k],
            device_id={"seq": h},
        )

    def own1(a):
        return pltpu.make_async_copy(tile_of(a, me), first[a].at[slot_of(me)], own_sem.at[a])

    def place_at(a):
        top, head = tile(me)
        return landing.at[a, my_block, head, pl.ds(0, most_pages), top]

    def hand2(a, k):
        d = lax.rem(me + k, n)
        return pltpu.make_async_remote_copy(
            src_ref=second.at[a, pl.ds(d * most_pages, most_pages)],
            dst_ref=place_at(a),
            send_sem=send2.at[a, k],
            recv_sem=recv2.at[a, k],
            device_id={"seq": d},
        )

    def own2(a):
        return pltpu.make_async_copy(
            second.at[a, pl.ds(me * most_pages, most_pages)], place_at(a), own_sem.at[2 + a]
        )

    pl.semaphore_wait(barrier, n - 1)
    for a in range(2):
        loads[a].wait()

        @each(1, spread)
        def _(k, a=a):
            hand1(a, k).start()

        own1(a).start()

    for copy in loads[7:]:
        copy.wait()
    running = jnp.int32(0)
    my_length = jnp.int32(0)
    my_slot = jnp.int32(0)
    for t in range(turns):
        start_s[t] = running
        length = lengths_ref[t]
        slot = slots_ref[t]
        own = lax.div(slot, slots_here) == me
        my_length = jnp.where(own, length, my_length)
        my_slot = jnp.where(own, lax.rem(slot, slots_here), my_slot)
        running = running + lax.div(length + (page_rows - 1), page_rows)

    @pl.loop(0, n)
    def _(d):
        begin = jnp.int32(0)
        for t in range(turns):
            begin = jnp.where(lax.div(slots_ref[t], slots_here) == d, start_s[t], begin)
        for j in range(most_pages):
            page = jnp.minimum(begin + j, group_pages * n - 1)
            row = lax.rem(lax.rem(page, n), spread) * group_pages + lax.div(page, n)
            pick_s[d * most_pages + j] = row

    loads[2].wait()
    for s in range(steps):
        qf[pl.ds(s * slots_here, slots_here), :] = q_v[s].astype(F32)
    qb[...] = qf[...].astype(BF16)

    tokens = pages_here * page_rows
    col = lax.broadcasted_iota(jnp.int32, (1, tokens), 1)
    col_page = col // page_rows
    col_row = col % page_rows
    lines = []
    for r in range(slots_here):
        room = jnp.zeros((1, tokens), jnp.int32)
        for c in range(cache_pages):
            left_over = cached_ref[r] - c * page_rows
            room = jnp.where(col_page == table_ref[r, c], left_over, room)
        lines.append(jnp.where(col_row < room, 0.0, NEG).astype(F32))
    bias = jnp.concatenate(lines * (rows_sr // slots_here), axis=0)

    def resident(g):
        keys = pk_v[:, :, pl.ds(g * HD, HD)].reshape(tokens, HD)
        values = pv_v[:, :, pl.ds(g * HD, HD)].reshape(tokens, HD)
        score = scores_of(qb, g, keys, bias)
        largest = jnp.max(score, axis=-1, keepdims=True)
        prob = jnp.exp2(score - largest)
        mx[:, g : g + 1] = largest
        sm[:, g : g + 1] = jnp.sum(prob, axis=-1, keepdims=True)
        acc[g] = jnp.dot(prob.astype(BF16), values, preferred_element_type=F32)

    loads[3].wait()
    loads[4].wait()
    for g in range(KVH):
        resident(g)

    loads[5].wait()
    loads[6].wait()
    for a in range(2):
        rows = jnp.concatenate([n_v[a, s].astype(F32) for s in range(steps)], axis=0).astype(BF16)
        for g in range(KVH):
            fresh[a, g, most_pages] = rows[:, g * HD : (g + 1) * HD]
    extra = fresh_span + rows_sr
    line = lax.broadcasted_iota(jnp.int32, (rows_sr, extra), 0)
    col = lax.broadcasted_iota(jnp.int32, (rows_sr, extra), 1)
    line_slot, line_step = line % slots_here, line // slots_here
    new_at = jnp.maximum(col - fresh_span, 0)
    fine_fresh = (line_slot == my_slot) & (col < my_length)
    fine_new = (
        (col >= fresh_span)
        & (new_at % slots_here == line_slot)
        & (new_at // slots_here <= line_step)
    )
    bias2_ref[...] = jnp.where(fine_fresh | fine_new, 0.0, NEG).astype(F32)

    def pass_on(a):
        @each(1, spread)
        def _(k):
            hand1(a, k).wait_recv()

        own1(a).wait()
        for i in range(n * most_pages):
            second[a, i] = first[a][pick_s[i]]

        @each(1, n)
        def _(k):
            hand2(a, k).start()

        own2(a).start()

    def arrive(a):
        @each(1, n)
        def _(k):
            hand2(a, k).wait_recv()

        own2(a).wait()
        if blocks > 1:
            begin = jnp.int32(0)
            for t in range(turns):
                begin = jnp.where(lax.div(slots_ref[t], slots_here) == me, start_s[t], begin)
            for j in range(most_pages):
                page = jnp.minimum(begin + j, group_pages * n - 1)
                block = lax.div(lax.rem(page, n), spread)
                for g in range(KVH):
                    fresh[a, g, j] = landing[a, block, g, j]

    place = lax.broadcasted_iota(jnp.int32, (page_rows, HD), 0)

    def land(a, ref, g):
        for j in range(most_pages):
            page = fresh[a, g, j].astype(F32)
            kept = jnp.where(place + j * page_rows < my_length, page, 0.0)
            ref[j, :, pl.ds(g * HD, HD)] = kept.astype(BF16)

    pass_on(0)
    pass_on(1)
    arrive(0)
    bias2 = bias2_ref[...]
    for g in range(KVH):
        score = scores_of(qb, g, fresh[0, g].reshape(extra, HD), bias2)
        before = mx[:, g : g + 1]
        largest = jnp.maximum(before, jnp.max(score, axis=-1, keepdims=True))
        prob = jnp.exp2(score - largest)
        shrink = jnp.exp2(before - largest)
        sm[:, g : g + 1] = sm[:, g : g + 1] * shrink + jnp.sum(prob, axis=-1, keepdims=True)
        acc[g] = acc[g] * shrink
        pf[g] = prob.astype(BF16)
        land(0, lk_ref, g)

    arrive(1)
    for g in range(KVH):
        values = fresh[1, g].reshape(extra, HD)
        mixed = acc[g] + jnp.dot(pf[g], values, preferred_element_type=F32)
        result = mixed / sm[:, g : g + 1]
        for e in range(share):
            qf[:, pl.ds((g * share + e) * HD, HD)] = result[e * rows_sr : (e + 1) * rows_sr]
        land(1, lv_ref, g)
    for s in range(steps):
        out_ref[s] = qf[pl.ds(s * slots_here, slots_here), :].astype(BF16)

    for a in range(2):

        @each(1, spread)
        def _(k, a=a):
            hand1(a, k).wait_send()

        @each(1, n)
        def _(k, a=a):
            hand2(a, k).wait_send()


def store(a_ref, b_ref, c_ref, a_hbm, b_hbm, c_hbm, sem):
    copies = [
        pltpu.make_async_copy(src, dst, sem.at[i])
        for i, (src, dst) in enumerate(((a_ref, a_hbm), (b_ref, b_hbm), (c_ref, c_hbm)))
    ]
    for copy in copies:
        copy.start()
    for copy in copies:
        copy.wait()


def per_device(
    queries,
    new_keys,
    new_values,
    pool_keys,
    pool_values,
    page_table,
    cached_len,
    turn_keys,
    turn_values,
    turn_lengths,
    turn_slot,
):
    n = lax.axis_size("seq")
    steps, slots_here, query_width = queries.shape
    pages_here, page_rows, kv_width = pool_keys.shape
    group_pages = turn_keys.shape[0]
    most_pages = -(-MOSTT // page_rows)
    spread = (page_rows // SUB) * (kv_width // HD)
    blocks = n // spread
    rows_sr = steps * slots_here
    rows = rows_sr * (QH // KVH)
    paged = (group_pages, page_rows, kv_width)
    hbm = pl.BlockSpec(memory_space=pltpu.HBM)
    vmem = pl.BlockSpec(memory_space=pltpu.VMEM)
    extra = most_pages * page_rows + rows_sr
    landed = jax.ShapeDtypeStruct((most_pages, page_rows, kv_width), BF16)
    outs = (jax.ShapeDtypeStruct(queries.shape, BF16), landed, landed)
    held = [
        pltpu.with_memory_space_constraint(x, pltpu.HBM)
        for x in (
            page_table,
            cached_len,
            turn_lengths,
            turn_slot,
            queries,
            new_keys,
            new_values,
            pool_keys,
            pool_values,
            turn_keys.reshape(paged),
            turn_values.reshape(paged),
        )
    ]
    parts = pl.pallas_call(
        functools.partial(kernel, n),
        out_shape=outs,
        in_specs=[hbm] * 11,
        out_specs=(vmem,) * 3,
        scratch_shapes=[
            pltpu.VMEM((rows_sr, query_width), BF16),
            pltpu.VMEM((KVH, rows, HD), F32),
            pltpu.VMEM((rows, KVH), F32),
            pltpu.VMEM((rows, KVH), F32),
            pltpu.VMEM((KVH, rows, extra), BF16),
            pltpu.VMEM((rows_sr, extra), F32),
            pltpu.VMEM(queries.shape, BF16),
            pltpu.VMEM((2,) + new_keys.shape, BF16),
            pltpu.VMEM(pool_keys.shape, BF16),
            pltpu.VMEM(pool_values.shape, BF16),
            pltpu.VMEM((2,) + paged, BF16),
            pltpu.VMEM((spread * group_pages, SUB, HD), BF16),
            pltpu.VMEM((spread * group_pages, SUB, HD), BF16),
            pltpu.VMEM((2, n * most_pages, SUB, HD), BF16),
            pltpu.VMEM((2, blocks, KVH, most_pages + 1, page_rows, HD), BF16),
            pltpu.VMEM((2, KVH, most_pages + 1, page_rows, HD) if blocks > 1 else (8, HD), BF16),
            pltpu.VMEM((rows_sr, query_width), F32),
            pltpu.SMEM(page_table.shape, jnp.int32),
            pltpu.SMEM(cached_len.shape, jnp.int32),
            pltpu.SMEM(turn_lengths.shape, jnp.int32),
            pltpu.SMEM(turn_slot.shape, jnp.int32),
            pltpu.SMEM(turn_lengths.shape, jnp.int32),
            pltpu.SMEM((n * most_pages,), jnp.int32),
            pltpu.SemaphoreType.DMA((11,)),
            pltpu.SemaphoreType.DMA((4,)),
            pltpu.SemaphoreType.DMA((2, spread)),
            pltpu.SemaphoreType.DMA((2, spread)),
            pltpu.SemaphoreType.DMA((2, n)),
            pltpu.SemaphoreType.DMA((2, n)),
        ],
        compiler_params=pltpu.CompilerParams(
            collective_id=0, has_side_effects=True, vmem_limit_bytes=24 * 1024 * 1024
        ),
    )(*held)
    attended, landed_keys, landed_values = pl.pallas_call(
        store,
        out_shape=outs,
        in_specs=[vmem] * 3,
        out_specs=(hbm,) * 3,
        scratch_shapes=[pltpu.SemaphoreType.DMA((3,))],
        compiler_params=pltpu.CompilerParams(vmem_limit_bytes=8 * 1024 * 1024),
    )(*parts)
    span = most_pages * page_rows
    return (
        attended,
        landed_keys.reshape(1, span, kv_width),
        landed_values.reshape(1, span, kv_width),
    )


def solution(mesh):
    in_specs = (
        P(None, ("groups", "seq"), None),
        P(None, ("groups", "seq"), None),
        P(None, ("groups", "seq"), None),
        P(("groups", "seq"), None, None),
        P(("groups", "seq"), None, None),
        P(("groups", "seq"), None),
        P(("groups", "seq")),
        P(None, ("groups", "seq"), None, None),
        P(None, ("groups", "seq"), None, None),
        P("groups"),
        P("groups"),
    )
    out_specs = (
        P(None, ("groups", "seq"), None),
        P(("groups", "seq"), None, None),
        P(("groups", "seq"), None, None),
    )
    return jax.shard_map(
        per_device, mesh=mesh, in_specs=in_specs, out_specs=out_specs, check_vma=False
    )
```

```python
import functools
import math

import jax
import jax.numpy as jnp
from jax import lax
from jax.experimental import pallas as pl
from jax.experimental.pallas import tpu as pltpu
from jax.sharding import PartitionSpec as P

QH = 64
KVH = 8
HD = 128
MOSTT = 80
SUB = 8
PLANE = 4
NEG = -1e30
F32 = jnp.float32
BF16 = jnp.bfloat16

FACTOR = math.log2(math.e) / math.sqrt(HD)


def scores_of(qb, g, keys, biases):
    share = QH // KVH
    parts = [qb[:, pl.ds((g * share + e) * HD, HD)] for e in range(share)]
    rows = jnp.concatenate(parts, axis=0)
    raw = lax.dot_general(rows, keys, (((1,), (1,)), ((), ())), preferred_element_type=F32)
    shaped = raw.reshape(share, biases.shape[0], keys.shape[0]) * FACTOR + biases[None]
    return shaped.reshape(rows.shape[0], keys.shape[0])


def each(first, last):
    if last - first > 32:
        return pl.loop(first, last)

    def run(body):
        for k in range(first, last):
            body(k)

    return run


def kernel(
    n,
    table_hbm,
    cached_hbm,
    lengths_hbm,
    slots_hbm,
    q_hbm,
    nk_hbm,
    nv_hbm,
    pk_hbm,
    pv_hbm,
    tk_hbm,
    tv_hbm,
    out_ref,
    lk_ref,
    lv_ref,
    qb,
    acc,
    mx,
    sm,
    pf,
    bias2_ref,
    q_v,
    n_v,
    pk_v,
    pv_v,
    t_v,
    first_k,
    first_v,
    second,
    landing,
    fresh,
    qf,
    table_ref,
    cached_ref,
    lengths_ref,
    slots_ref,
    start_s,
    pick_s,
    load_sem,
    own_sem,
    ready,
    send1,
    recv1,
    send2,
    recv2,
):
    me = lax.axis_index("seq")
    steps, slots_here, _ = q_hbm.shape
    group_pages, page_rows, kv_width = tk_hbm.shape
    pages_here = pk_hbm.shape[0]
    turns = lengths_ref.shape[0]
    cache_pages = table_ref.shape[1]
    lane_tiles = kv_width // HD
    spread = (page_rows // SUB) * lane_tiles
    most_pages = -(-MOSTT // page_rows)
    fresh_span = most_pages * page_rows
    blocks = n // spread
    rows_sr = steps * slots_here
    share = QH // KVH
    my_block = me // spread
    first = (first_k, first_v)
    if blocks == 1:
        fresh = landing.at[:, 0]

    barrier = pltpu.get_barrier_semaphore()

    @pl.loop(me + 1, n)
    def _(d):
        pl.semaphore_signal(barrier, inc=1, device_id={"seq": d})

    def load(index, src, dst):
        return pltpu.make_async_copy(src, dst, load_sem.at[index])

    loads = [
        load(0, tk_hbm, t_v.at[0]),
        load(1, tv_hbm, t_v.at[1]),
        load(2, q_hbm, q_v),
        load(3, pk_hbm, pk_v),
        load(4, pv_hbm, pv_v),
        load(5, nk_hbm, n_v.at[0]),
        load(6, nv_hbm, n_v.at[1]),
        load(7, lengths_hbm, lengths_ref),
        load(8, slots_hbm, slots_ref),
        load(9, table_hbm, table_ref),
        load(10, cached_hbm, cached_ref),
    ]
    for copy in loads:
        copy.start()

    def tile(h):
        t = lax.rem(h, spread)
        top = pl.multiple_of(lax.div(t, lane_tiles) * SUB, SUB)
        return pl.ds(top, SUB), lax.rem(t, lane_tiles)

    def tile_of(a, h):
        top, head = tile(h)
        return t_v.at[a, :, top, pl.ds(pl.multiple_of(head * HD, HD), HD)]

    def slot_of(src):
        return pl.ds(lax.rem(src, spread) * group_pages, group_pages)

    def hand1(a, h, src):
        return pltpu.make_async_remote_copy(
            src_ref=tile_of(a, h),
            dst_ref=first[a].at[slot_of(me)],
            send_sem=send1.at[a, lax.rem(h, spread)],
            recv_sem=recv1.at[a, lax.rem(src, spread)],
            device_id={"seq": h},
        )

    def own1(a):
        return pltpu.make_async_copy(tile_of(a, me), first[a].at[slot_of(me)], own_sem.at[a])

    def place_at(a):
        top, head = tile(me)
        return landing.at[a, my_block, head, pl.ds(0, most_pages), top]

    def hand2(a, d, src):
        return pltpu.make_async_remote_copy(
            src_ref=second.at[a, pl.ds(d * most_pages, most_pages)],
            dst_ref=place_at(a),
            send_sem=send2.at[a, d],
            recv_sem=recv2.at[a, src],
            device_id={"seq": d},
        )

    def own2(a):
        return pltpu.make_async_copy(
            second.at[a, pl.ds(me * most_pages, most_pages)], place_at(a), own_sem.at[2 + a]
        )

    start_block = my_block * spread
    my_plane = me // PLANE
    in_plane = lax.rem(me, PLANE)

    def partner(i):
        return (i // PLANE) * PLANE + lax.rem(in_plane + i, PLANE)

    def below(first_device, act):
        @pl.loop(first_device, my_plane * PLANE)
        def _(i):
            act(partner(i))

        for k in range(1, PLANE):
            d = partner(my_plane * PLANE + k)
            pl.when(d < me)(functools.partial(act, d))

    def above(last_device, act):
        for k in range(1, PLANE):
            d = partner(my_plane * PLANE + k)
            pl.when(d > me)(functools.partial(act, d))

        @pl.loop((my_plane + 1) * PLANE, last_device)
        def _(i):
            act(partner(i))

    def tell(d):
        pl.semaphore_signal(ready.at[me], inc=1, device_id={"seq": d})

    def send1_to(a):
        def act(d):
            hand1(a, d, me).start()

        return act

    def send1_ready(a):
        def act(d):
            pl.semaphore_wait(ready.at[d], 1)
            hand1(a, d, me).start()

        return act

    @pl.when(me > 0)
    def _():
        pl.semaphore_wait(barrier, me)

    below(0, tell)
    loads[0].wait()
    below(start_block, send1_to(0))
    own1(0).start()

    for copy in loads[7:]:
        copy.wait()
    running = jnp.int32(0)
    my_length = jnp.int32(0)
    my_slot = jnp.int32(0)
    for t in range(turns):
        start_s[t] = running
        length = lengths_ref[t]
        slot = slots_ref[t]
        own = lax.div(slot, slots_here) == me
        my_length = jnp.where(own, length, my_length)
        my_slot = jnp.where(own, lax.rem(slot, slots_here), my_slot)
        running = running + lax.div(length + (page_rows - 1), page_rows)

    @pl.loop(0, n)
    def _(d):
        begin = jnp.int32(0)
        for t in range(turns):
            begin = jnp.where(lax.div(slots_ref[t], slots_here) == d, start_s[t], begin)
        for j in range(most_pages):
            page = jnp.minimum(begin + j, group_pages * n - 1)
            row = lax.rem(lax.rem(page, n), spread) * group_pages + lax.div(page, n)
            pick_s[d * most_pages + j] = row

    loads[2].wait()
    for s in range(steps):
        qf[pl.ds(s * slots_here, slots_here), :] = q_v[s].astype(F32)
    qb[...] = qf[...].astype(BF16)

    tokens = pages_here * page_rows
    col = lax.broadcasted_iota(jnp.int32, (1, tokens), 1)
    col_page = col // page_rows
    col_row = col % page_rows
    lines = []
    for r in range(slots_here):
        room = jnp.zeros((1, tokens), jnp.int32)
        for c in range(cache_pages):
            left_over = cached_ref[r] - c * page_rows
            room = jnp.where(col_page == table_ref[r, c], left_over, room)
        lines.append(jnp.where(col_row < room, 0.0, NEG).astype(F32))
    bias = jnp.concatenate(lines * (rows_sr // slots_here), axis=0)

    def resident(g):
        keys = pk_v[:, :, pl.ds(g * HD, HD)].reshape(tokens, HD)
        values = pv_v[:, :, pl.ds(g * HD, HD)].reshape(tokens, HD)
        score = scores_of(qb, g, keys, bias)
        largest = jnp.max(score, axis=-1, keepdims=True)
        prob = jnp.exp2(score - largest)
        mx[:, g : g + 1] = largest
        sm[:, g : g + 1] = jnp.sum(prob, axis=-1, keepdims=True)
        acc[g] = jnp.dot(prob.astype(BF16), values, preferred_element_type=F32)

    loads[3].wait()
    loads[4].wait()
    above(start_block + spread, send1_ready(0))
    loads[1].wait()
    below(start_block, send1_to(1))
    above(start_block + spread, send1_to(1))
    own1(1).start()
    if blocks > 1:

        @pl.loop(start_block + spread, n)
        def _(d):
            pl.semaphore_wait(ready.at[d], 1)

    for g in range(KVH):
        resident(g)

    loads[5].wait()
    loads[6].wait()
    for a in range(2):
        rows = jnp.concatenate([n_v[a, s].astype(F32) for s in range(steps)], axis=0).astype(BF16)
        for g in range(KVH):
            fresh[a, g, most_pages] = rows[:, g * HD : (g + 1) * HD]
    extra = fresh_span + rows_sr
    line = lax.broadcasted_iota(jnp.int32, (rows_sr, extra), 0)
    col = lax.broadcasted_iota(jnp.int32, (rows_sr, extra), 1)
    line_slot, line_step = line % slots_here, line // slots_here
    new_at = jnp.maximum(col - fresh_span, 0)
    fine_fresh = (line_slot == my_slot) & (col < my_length)
    fine_new = (
        (col >= fresh_span)
        & (new_at % slots_here == line_slot)
        & (new_at // slots_here <= line_step)
    )
    bias2_ref[...] = jnp.where(fine_fresh | fine_new, 0.0, NEG).astype(F32)

    def pass_on(a):
        @each(1, spread)
        def _(k):
            src = start_block + lax.rem(lax.rem(me, spread) + k, spread)
            hand1(a, src, src).wait_recv()

        own1(a).wait()
        for i in range(n * most_pages):
            second[a, i] = first[a][pick_s[i]]

        def act(d):
            hand2(a, d, me).start()

        for k in range(1, n):
            act(lax.rem(me + k, n))

        own2(a).start()

    def arrive(a):
        @each(1, n)
        def _(k):
            src = lax.rem(me + k, n)
            hand2(a, src, src).wait_recv()

        own2(a).wait()
        if blocks > 1:
            begin = jnp.int32(0)
            for t in range(turns):
                begin = jnp.where(lax.div(slots_ref[t], slots_here) == me, start_s[t], begin)
            for j in range(most_pages):
                page = jnp.minimum(begin + j, group_pages * n - 1)
                block = lax.div(lax.rem(page, n), spread)
                for g in range(KVH):
                    fresh[a, g, j] = landing[a, block, g, j]

    place = lax.broadcasted_iota(jnp.int32, (page_rows, HD), 0)

    def land(a, ref, g):
        for j in range(most_pages):
            page = fresh[a, g, j].astype(F32)
            kept = jnp.where(place + j * page_rows < my_length, page, 0.0)
            ref[j, :, pl.ds(g * HD, HD)] = kept.astype(BF16)

    pass_on(0)
    pass_on(1)
    arrive(0)
    bias2 = bias2_ref[...]
    for g in range(KVH):
        score = scores_of(qb, g, fresh[0, g].reshape(extra, HD), bias2)
        before = mx[:, g : g + 1]
        largest = jnp.maximum(before, jnp.max(score, axis=-1, keepdims=True))
        prob = jnp.exp2(score - largest)
        shrink = jnp.exp2(before - largest)
        sm[:, g : g + 1] = sm[:, g : g + 1] * shrink + jnp.sum(prob, axis=-1, keepdims=True)
        acc[g] = acc[g] * shrink
        pf[g] = prob.astype(BF16)
        land(0, lk_ref, g)

    arrive(1)
    for g in range(KVH):
        values = fresh[1, g].reshape(extra, HD)
        mixed = acc[g] + jnp.dot(pf[g], values, preferred_element_type=F32)
        result = mixed / sm[:, g : g + 1]
        for e in range(share):
            qf[:, pl.ds((g * share + e) * HD, HD)] = result[e * rows_sr : (e + 1) * rows_sr]
        land(1, lv_ref, g)
    for s in range(steps):
        out_ref[s] = qf[pl.ds(s * slots_here, slots_here), :].astype(BF16)

    for a in range(2):

        @each(1, spread)
        def _(k, a=a):
            h = start_block + lax.rem(lax.rem(me, spread) + k, spread)
            hand1(a, h, me).wait_send()

        @each(1, n)
        def _(k, a=a):
            hand2(a, lax.rem(me + k, n), me).wait_send()


def store(a_ref, b_ref, c_ref, a_hbm, b_hbm, c_hbm, sem):
    copies = [
        pltpu.make_async_copy(src, dst, sem.at[i])
        for i, (src, dst) in enumerate(((a_ref, a_hbm), (b_ref, b_hbm), (c_ref, c_hbm)))
    ]
    for copy in copies:
        copy.start()
    for copy in copies:
        copy.wait()


def per_device(
    queries,
    new_keys,
    new_values,
    pool_keys,
    pool_values,
    page_table,
    cached_len,
    turn_keys,
    turn_values,
    turn_lengths,
    turn_slot,
):
    n = lax.axis_size("seq")
    steps, slots_here, query_width = queries.shape
    pages_here, page_rows, kv_width = pool_keys.shape
    group_pages = turn_keys.shape[0]
    most_pages = -(-MOSTT // page_rows)
    spread = (page_rows // SUB) * (kv_width // HD)
    blocks = n // spread
    rows_sr = steps * slots_here
    rows = rows_sr * (QH // KVH)
    paged = (group_pages, page_rows, kv_width)
    hbm = pl.BlockSpec(memory_space=pltpu.HBM)
    vmem = pl.BlockSpec(memory_space=pltpu.VMEM)
    extra = most_pages * page_rows + rows_sr
    landed = jax.ShapeDtypeStruct((most_pages, page_rows, kv_width), BF16)
    outs = (jax.ShapeDtypeStruct(queries.shape, BF16), landed, landed)
    held = [
        pltpu.with_memory_space_constraint(x, pltpu.HBM)
        for x in (
            page_table,
            cached_len,
            turn_lengths,
            turn_slot,
            queries,
            new_keys,
            new_values,
            pool_keys,
            pool_values,
            turn_keys.reshape(paged),
            turn_values.reshape(paged),
        )
    ]
    parts = pl.pallas_call(
        functools.partial(kernel, n),
        out_shape=outs,
        in_specs=[hbm] * 11,
        out_specs=(vmem,) * 3,
        scratch_shapes=[
            pltpu.VMEM((rows_sr, query_width), BF16),
            pltpu.VMEM((KVH, rows, HD), F32),
            pltpu.VMEM((rows, KVH), F32),
            pltpu.VMEM((rows, KVH), F32),
            pltpu.VMEM((KVH, rows, extra), BF16),
            pltpu.VMEM((rows_sr, extra), F32),
            pltpu.VMEM(queries.shape, BF16),
            pltpu.VMEM((2,) + new_keys.shape, BF16),
            pltpu.VMEM(pool_keys.shape, BF16),
            pltpu.VMEM(pool_values.shape, BF16),
            pltpu.VMEM((2,) + paged, BF16),
            pltpu.VMEM((spread * group_pages, SUB, HD), BF16),
            pltpu.VMEM((spread * group_pages, SUB, HD), BF16),
            pltpu.VMEM((2, n * most_pages, SUB, HD), BF16),
            pltpu.VMEM((2, blocks, KVH, most_pages + 1, page_rows, HD), BF16),
            pltpu.VMEM((2, KVH, most_pages + 1, page_rows, HD) if blocks > 1 else (8, HD), BF16),
            pltpu.VMEM((rows_sr, query_width), F32),
            pltpu.SMEM(page_table.shape, jnp.int32),
            pltpu.SMEM(cached_len.shape, jnp.int32),
            pltpu.SMEM(turn_lengths.shape, jnp.int32),
            pltpu.SMEM(turn_slot.shape, jnp.int32),
            pltpu.SMEM(turn_lengths.shape, jnp.int32),
            pltpu.SMEM((n * most_pages,), jnp.int32),
            pltpu.SemaphoreType.DMA((11,)),
            pltpu.SemaphoreType.DMA((4,)),
            pltpu.SemaphoreType.REGULAR((n,)),
            pltpu.SemaphoreType.DMA((2, spread)),
            pltpu.SemaphoreType.DMA((2, spread)),
            pltpu.SemaphoreType.DMA((2, n)),
            pltpu.SemaphoreType.DMA((2, n)),
        ],
        compiler_params=pltpu.CompilerParams(
            collective_id=0, has_side_effects=True, vmem_limit_bytes=24 * 1024 * 1024
        ),
    )(*held)
    attended, landed_keys, landed_values = pl.pallas_call(
        store,
        out_shape=outs,
        in_specs=[vmem] * 3,
        out_specs=(hbm,) * 3,
        scratch_shapes=[pltpu.SemaphoreType.DMA((3,))],
        compiler_params=pltpu.CompilerParams(vmem_limit_bytes=8 * 1024 * 1024),
    )(*parts)
    span = most_pages * page_rows
    return (
        attended,
        landed_keys.reshape(1, span, kv_width),
        landed_values.reshape(1, span, kv_width),
    )


def solution(mesh):
    in_specs = (
        P(None, ("groups", "seq"), None),
        P(None, ("groups", "seq"), None),
        P(None, ("groups", "seq"), None),
        P(("groups", "seq"), None, None),
        P(("groups", "seq"), None, None),
        P(("groups", "seq"), None),
        P(("groups", "seq")),
        P(None, ("groups", "seq"), None, None),
        P(None, ("groups", "seq"), None, None),
        P("groups"),
        P("groups"),
    )
    out_specs = (
        P(None, ("groups", "seq"), None),
        P(("groups", "seq"), None, None),
        P(("groups", "seq"), None, None),
    )
    return jax.shard_map(
        per_device, mesh=mesh, in_specs=in_specs, out_specs=out_specs, check_vma=False
    )
```

```python
import functools
import math

import jax
import jax.numpy as jnp
from jax import lax
from jax.experimental import pallas as pl
from jax.experimental.pallas import tpu as pltpu
from jax.sharding import PartitionSpec as P

QH = 64
KVH = 8
HD = 128
MOSTT = 80
SUB = 8
PLANE = 4
NEG = -1e30
F32 = jnp.float32
BF16 = jnp.bfloat16

FACTOR = math.log2(math.e) / math.sqrt(HD)


def scores_of(qb, g, keys, biases):
    share = QH // KVH
    parts = [qb[:, pl.ds((g * share + e) * HD, HD)] for e in range(share)]
    rows = jnp.concatenate(parts, axis=0)
    raw = lax.dot_general(rows, keys, (((1,), (1,)), ((), ())), preferred_element_type=F32)
    shaped = raw.reshape(share, biases.shape[0], keys.shape[0]) * FACTOR + biases[None]
    return shaped.reshape(rows.shape[0], keys.shape[0])


def each(first, last):
    if last - first > 32:
        return pl.loop(first, last)

    def run(body):
        for k in range(first, last):
            body(k)

    return run


def kernel(
    n,
    table_hbm,
    cached_hbm,
    lengths_hbm,
    slots_hbm,
    q_hbm,
    nk_hbm,
    nv_hbm,
    pk_hbm,
    pv_hbm,
    tk_hbm,
    tv_hbm,
    out_ref,
    lk_ref,
    lv_ref,
    qb,
    acc,
    mx,
    sm,
    pf,
    bias2_ref,
    q_v,
    n_v,
    pk_v,
    pv_v,
    t_v,
    first_k,
    first_v,
    second,
    landing,
    fresh,
    qf,
    table_ref,
    cached_ref,
    lengths_ref,
    slots_ref,
    start_s,
    pick_s,
    load_sem,
    own_sem,
    ready,
    send1,
    recv1,
    send2,
    recv2,
):
    me = lax.axis_index("seq")
    steps, slots_here, _ = q_hbm.shape
    group_pages, page_rows, kv_width = tk_hbm.shape
    pages_here = pk_hbm.shape[0]
    turns = lengths_ref.shape[0]
    cache_pages = table_ref.shape[1]
    lane_tiles = kv_width // HD
    spread = (page_rows // SUB) * lane_tiles
    most_pages = -(-MOSTT // page_rows)
    fresh_span = most_pages * page_rows
    blocks = n // spread
    rows_sr = steps * slots_here
    share = QH // KVH
    my_block = me // spread
    first = (first_k, first_v)
    if blocks == 1:
        fresh = landing.at[:, 0]

    barrier = pltpu.get_barrier_semaphore()

    @pl.loop(me + 1, n)
    def _(d):
        pl.semaphore_signal(barrier, inc=1, device_id={"seq": d})

    def load(index, src, dst):
        return pltpu.make_async_copy(src, dst, load_sem.at[index])

    loads = [
        load(0, tk_hbm, t_v.at[0]),
        load(1, tv_hbm, t_v.at[1]),
        load(2, q_hbm, q_v),
        load(3, pk_hbm, pk_v),
        load(4, pv_hbm, pv_v),
        load(5, nk_hbm, n_v.at[0]),
        load(6, nv_hbm, n_v.at[1]),
        load(7, lengths_hbm, lengths_ref),
        load(8, slots_hbm, slots_ref),
        load(9, table_hbm, table_ref),
        load(10, cached_hbm, cached_ref),
    ]
    for copy in loads:
        copy.start()

    def tile(h):
        t = lax.rem(h, spread)
        top = pl.multiple_of(lax.div(t, lane_tiles) * SUB, SUB)
        return pl.ds(top, SUB), lax.rem(t, lane_tiles)

    def tile_of(a, h):
        top, head = tile(h)
        return t_v.at[a, :, top, pl.ds(pl.multiple_of(head * HD, HD), HD)]

    def slot_of(src):
        return pl.ds(lax.rem(src, spread) * group_pages, group_pages)

    def hand1(a, h, src):
        return pltpu.make_async_remote_copy(
            src_ref=tile_of(a, h),
            dst_ref=first[a].at[slot_of(me)],
            send_sem=send1.at[a, lax.rem(h, spread)],
            recv_sem=recv1.at[a, lax.rem(src, spread)],
            device_id={"seq": h},
        )

    def own1(a):
        return pltpu.make_async_copy(tile_of(a, me), first[a].at[slot_of(me)], own_sem.at[a])

    def place_at(a):
        top, head = tile(me)
        return landing.at[a, my_block, head, pl.ds(0, most_pages), top]

    def hand2(a, d, src):
        return pltpu.make_async_remote_copy(
            src_ref=second.at[a, pl.ds(d * most_pages, most_pages)],
            dst_ref=place_at(a),
            send_sem=send2.at[a, d],
            recv_sem=recv2.at[a, src],
            device_id={"seq": d},
        )

    def own2(a):
        return pltpu.make_async_copy(
            second.at[a, pl.ds(me * most_pages, most_pages)], place_at(a), own_sem.at[2 + a]
        )

    start_block = my_block * spread
    my_plane = me // PLANE
    in_plane = lax.rem(me, PLANE)

    def partner(i):
        return (i // PLANE) * PLANE + lax.rem(in_plane + i, PLANE)

    def below(first_device, act):
        @pl.loop(first_device, my_plane * PLANE)
        def _(i):
            act(partner(i))

        for k in range(1, PLANE):
            d = partner(my_plane * PLANE + k)
            pl.when(d < me)(functools.partial(act, d))

    def above(last_device, act):
        for k in range(1, PLANE):
            d = partner(my_plane * PLANE + k)
            pl.when(d > me)(functools.partial(act, d))

        @pl.loop((my_plane + 1) * PLANE, last_device)
        def _(i):
            act(partner(i))

    def tell(d):
        pl.semaphore_signal(ready.at[me], inc=1, device_id={"seq": d})

    def send1_to(a):
        def act(d):
            hand1(a, d, me).start()

        return act

    def send1_ready(a):
        def act(d):
            pl.semaphore_wait(ready.at[d], 1)
            hand1(a, d, me).start()

        return act

    @pl.when(me > 0)
    def _():
        pl.semaphore_wait(barrier, me)

    below(0, tell)
    loads[0].wait()
    below(start_block, send1_to(0))
    own1(0).start()

    for copy in loads[7:]:
        copy.wait()
    running = jnp.int32(0)
    my_length = jnp.int32(0)
    my_slot = jnp.int32(0)
    for t in range(turns):
        start_s[t] = running
        length = lengths_ref[t]
        slot = slots_ref[t]
        own = lax.div(slot, slots_here) == me
        my_length = jnp.where(own, length, my_length)
        my_slot = jnp.where(own, lax.rem(slot, slots_here), my_slot)
        running = running + lax.div(length + (page_rows - 1), page_rows)

    @pl.loop(0, n)
    def _(d):
        begin = jnp.int32(0)
        for t in range(turns):
            begin = jnp.where(lax.div(slots_ref[t], slots_here) == d, start_s[t], begin)
        for j in range(most_pages):
            page = jnp.minimum(begin + j, group_pages * n - 1)
            row = lax.rem(lax.rem(page, n), spread) * group_pages + lax.div(page, n)
            pick_s[d * most_pages + j] = row

    loads[2].wait()
    for s in range(steps):
        qf[pl.ds(s * slots_here, slots_here), :] = q_v[s].astype(F32)
    qb[...] = qf[...].astype(BF16)

    tokens = pages_here * page_rows
    col = lax.broadcasted_iota(jnp.int32, (1, tokens), 1)
    col_page = col // page_rows
    col_row = col % page_rows
    lines = []
    for r in range(slots_here):
        room = jnp.zeros((1, tokens), jnp.int32)
        for c in range(cache_pages):
            left_over = cached_ref[r] - c * page_rows
            room = jnp.where(col_page == table_ref[r, c], left_over, room)
        lines.append(jnp.where(col_row < room, 0.0, NEG).astype(F32))
    bias = jnp.concatenate(lines * (rows_sr // slots_here), axis=0)

    def resident(g):
        keys = pk_v[:, :, pl.ds(g * HD, HD)].reshape(tokens, HD)
        values = pv_v[:, :, pl.ds(g * HD, HD)].reshape(tokens, HD)
        score = scores_of(qb, g, keys, bias)
        largest = jnp.max(score, axis=-1, keepdims=True)
        prob = jnp.exp2(score - largest)
        mx[:, g : g + 1] = largest
        sm[:, g : g + 1] = jnp.sum(prob, axis=-1, keepdims=True)
        acc[g] = jnp.dot(prob.astype(BF16), values, preferred_element_type=F32)

    loads[3].wait()
    loads[4].wait()
    above(start_block + spread, send1_ready(0))
    loads[1].wait()
    below(start_block, send1_to(1))
    above(start_block + spread, send1_to(1))
    own1(1).start()
    if blocks > 1:

        @pl.loop(start_block + spread, n)
        def _(d):
            pl.semaphore_wait(ready.at[d], 1)

    for g in range(KVH):
        resident(g)

    loads[5].wait()
    loads[6].wait()
    for a in range(2):
        rows = jnp.concatenate([n_v[a, s].astype(F32) for s in range(steps)], axis=0).astype(BF16)
        for g in range(KVH):
            fresh[a, g, most_pages] = rows[:, g * HD : (g + 1) * HD]
    extra = fresh_span + rows_sr
    line = lax.broadcasted_iota(jnp.int32, (rows_sr, extra), 0)
    col = lax.broadcasted_iota(jnp.int32, (rows_sr, extra), 1)
    line_slot, line_step = line % slots_here, line // slots_here
    new_at = jnp.maximum(col - fresh_span, 0)
    fine_fresh = (line_slot == my_slot) & (col < my_length)
    fine_new = (
        (col >= fresh_span)
        & (new_at % slots_here == line_slot)
        & (new_at // slots_here <= line_step)
    )
    bias2_ref[...] = jnp.where(fine_fresh | fine_new, 0.0, NEG).astype(F32)

    def pass_on(a):
        @each(1, spread)
        def _(k):
            src = start_block + lax.rem(lax.rem(me, spread) + k, spread)
            hand1(a, src, src).wait_recv()

        own1(a).wait()
        for i in range(n * most_pages):
            second[a, i] = first[a][pick_s[i]]

        def act(d):
            hand2(a, d, me).start()

        for k in range(1, n):
            act(lax.rem(me + k, n))

        own2(a).start()

    def arrive(a):
        @each(1, n)
        def _(k):
            src = lax.rem(me + k, n)
            hand2(a, src, src).wait_recv()

        own2(a).wait()
        if blocks > 1:
            begin = jnp.int32(0)
            for t in range(turns):
                begin = jnp.where(lax.div(slots_ref[t], slots_here) == me, start_s[t], begin)
            for j in range(most_pages):
                page = jnp.minimum(begin + j, group_pages * n - 1)
                block = lax.div(lax.rem(page, n), spread)
                for g in range(KVH):
                    fresh[a, g, j] = landing[a, block, g, j]

    place = lax.broadcasted_iota(jnp.int32, (page_rows, HD), 0)

    def land(a, ref, g):
        for j in range(most_pages):
            page = fresh[a, g, j].astype(F32)
            kept = jnp.where(place + j * page_rows < my_length, page, 0.0)
            ref[j, :, pl.ds(g * HD, HD)] = kept.astype(BF16)

    pass_on(0)
    pass_on(1)
    arrive(0)
    bias2 = bias2_ref[...]
    for g in range(KVH):
        score = scores_of(qb, g, fresh[0, g].reshape(extra, HD), bias2)
        before = mx[:, g : g + 1]
        largest = jnp.maximum(before, jnp.max(score, axis=-1, keepdims=True))
        prob = jnp.exp2(score - largest)
        shrink = jnp.exp2(before - largest)
        sm[:, g : g + 1] = sm[:, g : g + 1] * shrink + jnp.sum(prob, axis=-1, keepdims=True)
        acc[g] = acc[g] * shrink
        pf[g] = prob.astype(BF16)
        land(0, lk_ref, g)

    if blocks > 1:
        arrive(1)
    else:
        own2(1).wait()
    for g in (0, 1, 2, 3, 4, 5, 6, 7):
        if blocks == 1 and g in {0: (0, 1, 2, 3), 4: (4, 5, 6, 7)}:
            for src in range(n):
                if src % lane_tiles in {0: (0, 1, 2, 3), 4: (4, 5, 6, 7)}[g]:
                    pl.when(src != me)(hand2(1, src, src).wait_recv)
        values = fresh[1, g].reshape(extra, HD)
        mixed = acc[g] + jnp.dot(pf[g], values, preferred_element_type=F32)
        result = mixed / sm[:, g : g + 1]
        for e in range(share):
            qf[:, pl.ds((g * share + e) * HD, HD)] = result[e * rows_sr : (e + 1) * rows_sr]
        land(1, lv_ref, g)
    for s in range(steps):
        out_ref[s] = qf[pl.ds(s * slots_here, slots_here), :].astype(BF16)

    for a in range(2):

        @each(1, spread)
        def _(k, a=a):
            h = start_block + lax.rem(lax.rem(me, spread) + k, spread)
            hand1(a, h, me).wait_send()

        @each(1, n)
        def _(k, a=a):
            hand2(a, lax.rem(me + k, n), me).wait_send()


def store(a_ref, b_ref, c_ref, a_hbm, b_hbm, c_hbm, sem):
    copies = [
        pltpu.make_async_copy(src, dst, sem.at[i])
        for i, (src, dst) in enumerate(((a_ref, a_hbm), (b_ref, b_hbm), (c_ref, c_hbm)))
    ]
    for copy in copies:
        copy.start()
    for copy in copies:
        copy.wait()


def per_device(
    queries,
    new_keys,
    new_values,
    pool_keys,
    pool_values,
    page_table,
    cached_len,
    turn_keys,
    turn_values,
    turn_lengths,
    turn_slot,
):
    n = lax.axis_size("seq")
    steps, slots_here, query_width = queries.shape
    pages_here, page_rows, kv_width = pool_keys.shape
    group_pages = turn_keys.shape[0]
    most_pages = -(-MOSTT // page_rows)
    spread = (page_rows // SUB) * (kv_width // HD)
    blocks = n // spread
    rows_sr = steps * slots_here
    rows = rows_sr * (QH // KVH)
    paged = (group_pages, page_rows, kv_width)
    hbm = pl.BlockSpec(memory_space=pltpu.HBM)
    vmem = pl.BlockSpec(memory_space=pltpu.VMEM)
    extra = most_pages * page_rows + rows_sr
    landed = jax.ShapeDtypeStruct((most_pages, page_rows, kv_width), BF16)
    outs = (jax.ShapeDtypeStruct(queries.shape, BF16), landed, landed)
    held = [
        pltpu.with_memory_space_constraint(x, pltpu.HBM)
        for x in (
            page_table,
            cached_len,
            turn_lengths,
            turn_slot,
            queries,
            new_keys,
            new_values,
            pool_keys,
            pool_values,
            turn_keys.reshape(paged),
            turn_values.reshape(paged),
        )
    ]
    parts = pl.pallas_call(
        functools.partial(kernel, n),
        out_shape=outs,
        in_specs=[hbm] * 11,
        out_specs=(vmem,) * 3,
        scratch_shapes=[
            pltpu.VMEM((rows_sr, query_width), BF16),
            pltpu.VMEM((KVH, rows, HD), F32),
            pltpu.VMEM((rows, KVH), F32),
            pltpu.VMEM((rows, KVH), F32),
            pltpu.VMEM((KVH, rows, extra), BF16),
            pltpu.VMEM((rows_sr, extra), F32),
            pltpu.VMEM(queries.shape, BF16),
            pltpu.VMEM((2,) + new_keys.shape, BF16),
            pltpu.VMEM(pool_keys.shape, BF16),
            pltpu.VMEM(pool_values.shape, BF16),
            pltpu.VMEM((2,) + paged, BF16),
            pltpu.VMEM((spread * group_pages, SUB, HD), BF16),
            pltpu.VMEM((spread * group_pages, SUB, HD), BF16),
            pltpu.VMEM((2, n * most_pages, SUB, HD), BF16),
            pltpu.VMEM((2, blocks, KVH, most_pages + 1, page_rows, HD), BF16),
            pltpu.VMEM((2, KVH, most_pages + 1, page_rows, HD) if blocks > 1 else (8, HD), BF16),
            pltpu.VMEM((rows_sr, query_width), F32),
            pltpu.SMEM(page_table.shape, jnp.int32),
            pltpu.SMEM(cached_len.shape, jnp.int32),
            pltpu.SMEM(turn_lengths.shape, jnp.int32),
            pltpu.SMEM(turn_slot.shape, jnp.int32),
            pltpu.SMEM(turn_lengths.shape, jnp.int32),
            pltpu.SMEM((n * most_pages,), jnp.int32),
            pltpu.SemaphoreType.DMA((11,)),
            pltpu.SemaphoreType.DMA((4,)),
            pltpu.SemaphoreType.REGULAR((n,)),
            pltpu.SemaphoreType.DMA((2, spread)),
            pltpu.SemaphoreType.DMA((2, spread)),
            pltpu.SemaphoreType.DMA((2, n)),
            pltpu.SemaphoreType.DMA((2, n)),
        ],
        compiler_params=pltpu.CompilerParams(
            collective_id=0, has_side_effects=True, vmem_limit_bytes=24 * 1024 * 1024
        ),
    )(*held)
    attended, landed_keys, landed_values = pl.pallas_call(
        store,
        out_shape=outs,
        in_specs=[vmem] * 3,
        out_specs=(hbm,) * 3,
        scratch_shapes=[pltpu.SemaphoreType.DMA((3,))],
        compiler_params=pltpu.CompilerParams(vmem_limit_bytes=8 * 1024 * 1024),
    )(*parts)
    span = most_pages * page_rows
    return (
        attended,
        landed_keys.reshape(1, span, kv_width),
        landed_values.reshape(1, span, kv_width),
    )


def solution(mesh):
    in_specs = (
        P(None, ("groups", "seq"), None),
        P(None, ("groups", "seq"), None),
        P(None, ("groups", "seq"), None),
        P(("groups", "seq"), None, None),
        P(("groups", "seq"), None, None),
        P(("groups", "seq"), None),
        P(("groups", "seq")),
        P(None, ("groups", "seq"), None, None),
        P(None, ("groups", "seq"), None, None),
        P("groups"),
        P("groups"),
    )
    out_specs = (
        P(None, ("groups", "seq"), None),
        P(("groups", "seq"), None, None),
        P(("groups", "seq"), None, None),
    )
    return jax.shard_map(
        per_device, mesh=mesh, in_specs=in_specs, out_specs=out_specs, check_vma=False
    )
```
